256 devices in a mesh: tok: 16 (over z, core), voc: 16 (over x, y).
Axes of the slice: x: 4, y: 4, z: 8, core: 2. Of those that a mesh axis runs over, the one named last changes fastest.
Arguments:
- hidden: bfloat16 [8192, 1024], P('tok'), may hold values from -64 to 64
- head_weight: bfloat16 [1024, 65536], P('tok', 'voc'), may hold values from -1 to 1
- target_logits: bfloat16 [8192, 65536], P('tok', 'voc'), may hold values from -320 to 320
- token_ids: int32 [8192], P('tok'), may hold values from 0 to 65535
Outputs:
- loss: float32 [], replicated
- grad_hidden: float32 [8192, 1024], P('tok', 'voc')
- grad_head: float32 [1024, 65536], P('tok', 'voc')
The draws below stay inside these ranges and needn't reach their ends.
All inputs are finite; a program needn't handle non-finite values.
Results may differ from the reference program's by a relative error of at most 0.015.
Values may be sent and summed in bfloat16 or wider, within the bound.
A program may use at most 128 MiB of HBM per device.

```python
import math
import jax
import jax.numpy as jnp
import numpy as np
from jax import lax

DH = 1024
TOK_DEV = 512
VOCAB = 65536
TOKENS = 8192
N_TOK = 16


def weight_table(key):
    return jax.random.normal(jax.random.fold_in(key, 11), (DH, VOCAB), jnp.float32) / math.sqrt(DH)


def row_rise(top):
    return jnp.exp(jnp.linspace(0.0, math.log(top), TOKENS)).astype(jnp.float32)[:, None]


def draw_head_weight(key, part):
    return jnp.clip(weight_table(key), -1.0, 1.0).astype(jnp.bfloat16)


def draw_hidden(key, part):
    base = 1.5 * row_rise(4.0) * jax.random.normal(jax.random.fold_in(key, 21), (TOKENS, DH), jnp.float32)
    return jnp.clip(base, -64.0, 64.0).astype(jnp.bfloat16)


def draw_target_logits(key, part):
    base = 1.5 * row_rise(4.0) * jax.random.normal(jax.random.fold_in(key, 31), (TOKENS, VOCAB), jnp.float32)
    return jnp.clip(base, -320.0, 320.0).astype(jnp.bfloat16)


def touch_ends(result, key, smallest, top_value):
    spot = [jax.random.randint(jax.random.fold_in(key, axis), (), 0, length) for axis, length in enumerate(result.shape)]
    main_axis = result.shape.index(max(result.shape))
    next_to = spot[:main_axis] + [(spot[main_axis] + 1) % result.shape[main_axis]] + spot[main_axis + 1:]
    return result.at[tuple(spot)].set(smallest).at[tuple(next_to)].set(top_value)


def rank_table(count, skew):
    weights = [(1 << 20) // math.isqrt(grade ** skew) + 1 for grade in range(1, count + 1)]
    spread = 1 + sum(weights) // (1 << 30)
    return np.cumsum(np.array([max(1, weight // spread) for weight in weights]))


def skewed_ids(own_key, dims, number_of, lean):
    table = rank_table(number_of, lean)
    pick = jax.random.randint(jax.random.fold_in(own_key, 1), dims, 0, int(table[number_of - 1]))
    standing = jnp.searchsorted(jnp.asarray(table, jnp.int32), pick, side="right")
    return jax.random.permutation(jax.random.fold_in(own_key, 2), number_of)[standing].astype(jnp.int32)


def setup_inputs(seed: int = 0) -> dict:
    key_list = jax.random.split(jax.random.key(seed), 5)
    return {
        "hidden": draw_hidden(jax.random.fold_in(key_list[4], 71), 0),
        "head_weight": draw_head_weight(jax.random.fold_in(key_list[4], 71), 0),
        "target_logits": draw_target_logits(jax.random.fold_in(key_list[4], 71), 0),
        "token_ids": touch_ends(skewed_ids(key_list[3], (TOKENS,), VOCAB, 2), jax.random.fold_in(key_list[3], 3), 0, VOCAB - 1).astype(jnp.int32),
    }


ce_weight = 0.5


def block_terms(head, hid, target, ids):
    draft = jnp.dot(hid, head, preferred_element_type=jnp.float32)
    target = target.astype(jnp.float32)
    draft_max = jnp.max(draft, axis=1, keepdims=True)
    target_max = jnp.max(target, axis=1, keepdims=True)
    draft_exp = jnp.exp(draft - draft_max)
    target_exp = jnp.exp(target - target_max)
    draft_sum = jnp.sum(draft_exp, axis=1, keepdims=True)
    target_sum = jnp.sum(target_exp, axis=1, keepdims=True)
    probs_q = draft_exp / draft_sum
    probs_p = target_exp / target_sum
    log_q = draft - draft_max - jnp.log(draft_sum)
    log_p = target - target_max - jnp.log(target_sum)
    column = lax.broadcasted_iota(jnp.int32, draft.shape, 1)
    own = (column == ids[:, None].astype(jnp.int32)).astype(jnp.float32)
    kl_part = jnp.sum(probs_p * (log_p - log_q))
    ce_part = -jnp.sum(own * log_q)
    slope = ((1.0 + ce_weight) * probs_q - probs_p - ce_weight * own).astype(jnp.bfloat16)
    grad_hid = jnp.dot(slope, head.T, preferred_element_type=jnp.float32)
    grad_part = jnp.dot(hid.T, slope, preferred_element_type=jnp.float32).astype(jnp.bfloat16).astype(jnp.float32)
    return kl_part + ce_weight * ce_part, grad_hid, grad_part


def reference(hidden, head_weight, target_logits, token_ids):
    hid_blocks = hidden.reshape(N_TOK, TOK_DEV, DH)
    target_blocks = target_logits.reshape(N_TOK, TOK_DEV, VOCAB)
    id_blocks = token_ids.reshape(N_TOK, TOK_DEV)

    def step(carry, xs):
        total, grad_head = carry
        hid, target, ids = xs
        loss_part, grad_hid, grad_part = block_terms(head_weight, hid, target, ids)
        return (total + loss_part, grad_head + grad_part), grad_hid

    start = (jnp.zeros((), jnp.float32), jnp.zeros((DH, VOCAB), jnp.float32))
    (total, grad_head), grad_hidden = lax.scan(step, start, (hid_blocks, target_blocks, id_blocks))
    return total / TOKENS, grad_hidden.reshape(TOKENS, DH), grad_head
```

```python
import functools

import jax
import jax.numpy as jnp
from jax import lax
from jax.experimental import pallas as pl
from jax.experimental.pallas import tpu as pltpu
from jax.sharding import Mesh
from jax.sharding import PartitionSpec as P

VOC = ("voc_0", "voc_1")
TOK = ("tok_0", "tok_1")
CE = 0.5
F32 = jnp.float32
BF16 = jnp.bfloat16
MESH = pl.DeviceIdType.MESH
ROWS = 32
LOW = -1e30


def kernel(dims, *refs):
    Z, X, Y, T, D, V, NS = dims
    NV = X * Y
    NB = 2 * NS
    W = V // NB
    RB = D // (2 * Z)
    G = W // 128
    NE = (Z - 1) * NS
    NC = Z * NS
    (
        hid_hbm, head_hbm, tgt_hbm, ids_ref,
        loss_out, gh_out, gw_out,
        hg, hid, hid_t, tgt, zed, base, slope,
        part, sib_out, sib_in, ring_out, ring_in, gh_send, gh_recv,
        st_t, st_z, run_m, run_s, ids_c, m_c, s_c, own_t, lsum, row_t,
        l_xy, l_sib, l_z,
        in_sem, ag_s, ag_r, sb_s, sb_r, so_sem,
        rs_s, rs_r, rb_s, rb_r, gh_s, gh_r, tt_s, tt_r, zz_s, zz_r,
        lx_s, lx_r, lz_s, lz_r, lb_sem,
    ) = refs
    z = lax.axis_index("tok_0")
    c = lax.axis_index("tok_1")
    x = lax.axis_index("voc_0")
    y = lax.axis_index("voc_1")
    me = x * Y + y
    sib = 1 - c
    right = lax.rem(z + 1, Z)
    left = lax.rem(z + Z - 1, Z)
    toward = ({"tok_0": right}, {"tok_0": left})
    other = {"tok_1": sib}

    def plane(k):
        j = lax.rem(me + k, NV)
        return j, {"voc_0": j // Y, "voc_1": lax.rem(j, Y)}

    def remote(src, dst, s, r, device):
        return pltpu.make_async_remote_copy(
            src_ref=src, dst_ref=dst, send_sem=s, recv_sem=r, device_id=device, device_id_type=MESH
        )

    mine = 2 * z + c

    def in_head(b):
        return pltpu.make_async_copy(head_hbm.at[:, pl.ds(b * W, W)], hg.at[mine, b], in_sem.at[b])

    def in_hid(k):
        return pltpu.make_async_copy(
            hid_hbm.at[:, pl.ds(k * 2 * RB, 2 * RB)], hid.at[k], in_sem.at[NB + k]
        )

    def in_tgt(b):
        return pltpu.make_async_copy(
            tgt_hbm.at[:, pl.ds(b * W, W)], tgt.at[b], in_sem.at[NB + Z + b]
        )

    for b in range(NB):
        in_head(b).start()
    for k in range(Z):
        in_hid(k).start()
    for b in range(NB):
        in_tgt(b).start()

    barrier = pltpu.get_barrier_semaphore()
    for device in (*toward, other):
        pl.semaphore_signal(barrier, inc=1, device_id=device, device_id_type=MESH)
    for k in range(1, NV):
        pl.semaphore_signal(barrier, inc=1, device_id=plane(k)[1], device_id_type=MESH)
    pl.semaphore_wait(barrier, 3 + NV - 1)

    def chip_at(way, s):
        return lax.rem(z + Z - s, Z) if way == 0 else lax.rem(z + s, Z)

    def ag(way, n):
        slot = hg.at[2 * chip_at(way, n // NS) + c, way * NS + lax.rem(n, NS)]
        return remote(slot, slot, ag_s.at[way, n], ag_r.at[way, n], toward[way])

    def ag_in(way, n):
        slot = hg.at[2 * chip_at(way, n // NS + 1) + c, way * NS + lax.rem(n, NS)]
        return remote(slot, slot, ag_s.at[way, n], ag_r.at[way, n], toward[way])

    def sb(way, n, core):
        slot = hg.at[2 * chip_at(way, n // NS + 1) + core, way * NS + lax.rem(n, NS)]
        return remote(slot, slot, sb_s.at[way, n], sb_r.at[way, n], other)

    def shard(core):
        slot = hg.at[2 * z + core]
        return remote(slot, slot, so_sem.at[0], so_sem.at[1], other)

    for i in range(NS):
        for way in range(2):
            in_head(way * NS + i).wait()
            ag(way, i).start()
    shard(c).start()

    @pl.loop(0, NB)
    def _(b):
        zed[b] = jnp.zeros((T, W), F32)

    @pl.loop(0, Z)
    def _(k):
        in_hid(k).wait()
        hid_t[k] = hid[k].T

    def column(row):
        return jnp.broadcast_to(row, (128, T)).T

    ids_c[...] = column(ids_ref[...].astype(F32))

    def reset():
        run_m[...] = jnp.full((T, 128), LOW, F32)
        run_s[...] = jnp.zeros((T, 128), F32)

    reset()
    own_t[...] = jnp.zeros((ROWS, W), F32)
    lsum[...] = jnp.zeros((ROWS, W), F32)

    def groups(v):
        return [v[:, g * 128 : (g + 1) * 128] for g in range(G)]

    def stats(load):
        @pl.loop(0, T // ROWS)
        def _(k):
            at = pl.ds(pl.multiple_of(k * ROWS, ROWS), ROWS)
            cols = groups(load(at))
            old = run_m[at]
            new = functools.reduce(jnp.maximum, cols, old)
            total = run_s[at] * jnp.exp(old - new)
            run_s[at] = total + functools.reduce(jnp.add, [jnp.exp(v - new) for v in cols])
            run_m[at] = new

    def local_stats():
        m = run_m[...].T
        top = jnp.max(m, axis=0, keepdims=True)
        return top, jnp.sum(run_s[...].T * jnp.exp(m - top), axis=0, keepdims=True)

    def st(ref, s, r, k):
        return remote(ref.at[me], ref.at[me], s.at[k], r.at[me], plane(k)[1])

    def st_in(ref, s, r, k):
        j, device = plane(k)
        return remote(ref.at[j], ref.at[j], s.at[k], r.at[j], device)

    def send_stats(ref, s, r):
        top, total = local_stats()
        ref[me] = jnp.concatenate([top, total], axis=0)
        for k in range(1, NV):
            st(ref, s, r, k).start()

    def joined_stats(ref, s, r):
        for k in range(1, NV):
            st_in(ref, s, r, k).wait_recv()
        all_m = jnp.concatenate([ref[j][0:1] for j in range(NV)], axis=0)
        all_s = jnp.concatenate([ref[j][1:2] for j in range(NV)], axis=0)
        top = jnp.max(all_m, axis=0, keepdims=True)
        return top, jnp.sum(all_s * jnp.exp(all_m - top), axis=0, keepdims=True)

    lane = lax.broadcasted_iota(jnp.int32, (ROWS, W), 1)

    def wide(v):
        return jnp.concatenate([v] * G, axis=1)

    def fill_base(b):
        col = (lane + (me * V + b * W)).astype(F32)

        @pl.loop(0, T // ROWS)
        def _(k):
            at = pl.ds(pl.multiple_of(k * ROWS, ROWS), ROWS)
            t = tgt[b, at].astype(F32)
            p = jnp.exp(t - wide(m_c[at])) * wide(s_c[at])
            own = col == wide(ids_c[at])
            base[b, at] = jnp.where(own, p + CE, p)
            own_t[...] += jnp.where(own, t, 0.0)

    def draft(m):
        s = m // NS + 1
        for way in range(2):
            b = way * NS + lax.rem(m, NS)
            chips = (chip_at(way, s - 1), chip_at(way, s))
            lhs = jnp.concatenate([hid[k] for k in chips], axis=1)
            rhs = jnp.concatenate([hg[2 * k + e, b] for k in chips for e in range(2)], axis=0)
            zed[b] += jnp.dot(lhs, rhs, preferred_element_type=F32)

    def arrive(n):
        for way in range(2):
            ag_in(way, n).wait_recv()

            @pl.when(n + NS < NE)
            def _():
                ag(way, n + NS).start()

            sb(way, n, c).start()

    def arrived(m):
        for way in range(2):
            sb(way, m, sib).wait_recv()

    for b in range(NB):
        in_tgt(b).wait()
    shard(sib).wait_recv()

    LAST = NE - NS

    @pl.loop(0, LAST + 1)
    def _(n):
        arrive(n)
        s = n // NS + 1
        i = lax.rem(n, NS)

        @pl.when(n > 0)
        def _():
            arrived(n - 1)

        @pl.when((n > 0) & (lax.rem((n - 1) // NS, 2) == 0) & (n < LAST + 1))
        def _():
            draft(n - 1)

        @pl.when(s == 2)
        def _():
            for way in range(2):
                stats(lambda at: tgt[way * NS + i, at].astype(F32))

        @pl.when((s == 3) & (i == 0))
        def _():
            send_stats(st_t, tt_s, tt_r)
            reset()

        @pl.when((s == 4) & (i == NS - 1))
        def _():
            top, total = joined_stats(st_t, tt_s, tt_r)
            m_c[...] = column(top)
            s_c[...] = column(1.0 / total)
            row_t[...] = top + jnp.log(total)

        @pl.when(s == Z - 2)
        def _():
            for way in range(2):
                fill_base(way * NS + i)

    @pl.loop(LAST + 1, NE + 1)
    def _(n):
        @pl.when(n < NE)
        def _():
            arrive(n)

        arrived(n - 1)
        draft(n - 1)
        for way in range(2):
            b = way * NS + lax.rem(n - 1, NS)
            stats(lambda at: zed[b, at])

    send_stats(st_z, zz_s, zz_r)
    top_z, total_z = joined_stats(st_z, zz_s, zz_r)
    m_c[...] = column(top_z)
    s_c[...] = column((1.0 + CE) / total_z)
    row_t[...] = ((1.0 + CE) * (top_z + jnp.log(total_z)) - row_t[...]) * (1.0 / NV)

    def fill_slope(b):
        @pl.loop(0, T // ROWS)
        def _(k):
            at = pl.ds(pl.multiple_of(k * ROWS, ROWS), ROWS)
            q = jnp.exp(zed[b, at] - wide(m_c[at])) * wide(s_c[at])
            slope[b, at] = (q - base[b, at]).astype(BF16)

    def rb(way, n):
        return remote(
            sib_out.at[way, n], sib_in.at[way, n], rb_s.at[way, n], rb_r.at[way, n], other
        )

    def rs(way, n):
        return remote(
            ring_out.at[way, n], ring_in.at[way, n], rs_s.at[way, n], rs_r.at[way, n], toward[way]
        )

    def compute(n):
        s = n // NS
        slot = lax.rem(n, 2)
        for way in range(2):
            b = way * NS + lax.rem(n, NS)
            got = jnp.dot(hid_t[chip_at(way, s + 1)], slope[b], preferred_element_type=F32)
            part[slot, way, 0] = got[:RB]
            part[slot, way, 1] = got[RB:]
            sib_out[way, n] = part[slot, way, sib].astype(BF16)
            rb(way, n).start()

    def finish(n):
        s = n // NS
        slot = lax.rem(n, 2)
        for way in range(2):
            rb(way, n).wait_recv()

            @pl.when(s == 0)
            def _():
                val = part[slot, way, c] + sib_in[way, n].astype(F32)
                ring_out[way, n] = val.astype(BF16)
                rs(way, n).start()

            @pl.when(s > 0)
            def _():
                rs(way, n - NS).wait_recv()
                val = (part[slot, way, c] + sib_in[way, n].astype(F32)) + ring_in[
                    way, n - NS
                ].astype(F32)

                @pl.when(s < Z - 1)
                def _():
                    ring_out[way, n] = val.astype(BF16)
                    rs(way, n).start()

                @pl.when(s == Z - 1)
                def _():
                    b = way * NS + lax.rem(n, NS)
                    gw_out[:, pl.ds(pl.multiple_of(b * W, W), W)] = val

    def gh(j):
        device = {"voc_0": j // Y, "voc_1": lax.rem(j, Y)}
        return remote(gh_send.at[j], gh_recv.at[me], gh_s.at[j], gh_r.at[me], device)

    def gh_in(k):
        j, device = plane(k)
        return remote(gh_send.at[j], gh_recv.at[j], gh_s.at[j], gh_r.at[j], device)

    def hidden_part(e):
        r = lax.rem(e + me // 2, Z)
        acc = jnp.zeros((2 * RB, T), F32)
        for b in range(NB):
            lhs = jnp.concatenate([hg[2 * r, b], hg[2 * r + 1, b]], axis=0)
            acc = acc + lax.dot_general(
                lhs, slope[b], (((1,), (1,)), ((), ())), preferred_element_type=F32
            )
        for e2 in range(2):
            gh_send[2 * r + e2] = acc[e2 * RB : (e2 + 1) * RB].astype(BF16)

            @pl.when(2 * r + e2 != me)
            def _():
                gh(2 * r + e2).start()

    def loss_part(b):
        @pl.loop(0, T // ROWS)
        def _(k):
            at = pl.ds(pl.multiple_of(k * ROWS, ROWS), ROWS)
            lsum[...] += base[b, at] * (tgt[b, at].astype(F32) - zed[b, at])

    def total_of(v):
        return jnp.sum(jnp.sum(v, axis=0, keepdims=True), axis=1, keepdims=True)

    def sib_loss():
        return remote(l_sib.at[0], l_sib.at[1], lb_sem.at[0], lb_sem.at[1], other)

    def ring_loss(k):
        slot = l_z.at[chip_at(0, k)]
        return remote(slot, slot, lz_s.at[k], lz_r.at[k], toward[0])

    def ring_loss_in(k):
        slot = l_z.at[chip_at(0, k + 1)]
        return remote(slot, slot, lz_s.at[k], lz_r.at[k], toward[0])

    @pl.loop(0, NC + 1)
    def _(n):
        @pl.when(n < NS)
        def _():
            for way in range(2):
                fill_slope(way * NS + n)

        @pl.when(n < NC)
        def _():
            compute(n)

        @pl.when(n > 0)
        def _():
            finish(n - 1)

        @pl.when((n >= NS + 1) & (n < NS + 1 + 2 * Z) & (lax.rem(n - NS - 1, 2) == 0))
        def _():
            hidden_part((n - NS - 1) // 2)

        @pl.when((n >= NS) & (n < 2 * NS))
        def _():
            for way in range(2):
                loss_part(way * NS + lax.rem(n, NS))

        @pl.when(n == 2 * NS)
        def _():
            local = total_of(lsum[...] - CE * own_t[...]) + total_of(row_t[...])
            l_xy[me] = jnp.broadcast_to(local, (8, 128))
            for k in range(1, NV):
                st(l_xy, lx_s, lx_r, k).start()

        @pl.when(n == 3 * NS - 1)
        def _():
            for k in range(1, NV):
                st_in(l_xy, lx_s, lx_r, k).wait_recv()
            l_sib[0] = functools.reduce(jnp.add, [l_xy[j] for j in range(NV)])
            sib_loss().start()

        @pl.when(n == 3 * NS)
        def _():
            sib_loss().wait_recv()
            l_z[z] = l_sib[0] + l_sib[1]
            ring_loss(0).start()

        @pl.when((n > 3 * NS) & (n <= 3 * NS + 2 * (Z - 1)) & (lax.rem(n - 3 * NS, 2) == 0))
        def _():
            k = (n - 3 * NS) // 2
            ring_loss_in(k - 1).wait_recv()

            @pl.when(k < Z - 1)
            def _():
                ring_loss(k).start()

    loss_out[...] = functools.reduce(jnp.add, [l_z[k] for k in range(Z)]) * (1.0 / (2 * Z * T))
    for k in range(1, NV):
        gh_in(k).wait_recv()
    gh_recv[me] = gh_send[me]
    gh_out[...] = functools.reduce(jnp.add, [gh_recv[j].astype(F32) for j in range(NV)])

    shard(c).wait_send()
    sib_loss().wait_send()

    @pl.loop(0, NE)
    def _(n):
        for way in range(2):
            ag(way, n).wait_send()
            sb(way, n, c).wait_send()
            rs(way, n).wait_send()

    @pl.loop(0, NC)
    def _(n):
        for way in range(2):
            rb(way, n).wait_send()

    @pl.loop(0, Z - 1)
    def _(k):
        ring_loss(k).wait_send()

    for k in range(1, NV):
        st(st_t, tt_s, tt_r, k).wait_send()
        st(st_z, zz_s, zz_r, k).wait_send()
        st(l_xy, lx_s, lx_r, k).wait_send()
        gh_in(k).wait_send()


def body(dims, hidden, head, target, ids):
    Z, X, Y, T, D, V, NS = dims
    NV = X * Y
    NB = 2 * NS
    W = V // NB
    RB = D // (2 * Z)
    NE, NC = (Z - 1) * NS, Z * NS
    vmem, dma = pltpu.VMEM, pltpu.SemaphoreType.DMA
    hbm = pl.BlockSpec(memory_space=pltpu.HBM)
    local = pl.BlockSpec(memory_space=pltpu.VMEM)
    loss, gh, gw = pl.pallas_call(
        functools.partial(kernel, dims),
        out_shape=(
            jax.ShapeDtypeStruct((8, 128), F32),
            jax.ShapeDtypeStruct((RB, T), F32),
            jax.ShapeDtypeStruct((RB, V), F32),
        ),
        in_specs=[hbm, hbm, hbm, local],
        out_specs=(local, local, local),
        scratch_shapes=[
            vmem((2 * Z, NB, RB, W), BF16),
            vmem((Z, T, 2 * RB), BF16),
            vmem((Z, 2 * RB, T), BF16),
            vmem((NB, T, W), BF16),
            vmem((NB, T, W), F32),
            vmem((NB, T, W), F32),
            vmem((NB, T, W), BF16),
            vmem((2, 2, 2, RB, W), F32),
            vmem((2, NC, RB, W), BF16),
            vmem((2, NC, RB, W), BF16),
            vmem((2, NE, RB, W), BF16),
            vmem((2, NE, RB, W), BF16),
            vmem((NV, RB, T), BF16),
            vmem((NV, RB, T), BF16),
            vmem((NV, 2, T), F32),
            vmem((NV, 2, T), F32),
            vmem((T, 128), F32),
            vmem((T, 128), F32),
            vmem((T, 128), F32),
            vmem((T, 128), F32),
            vmem((T, 128), F32),
            vmem((ROWS, W), F32),
            vmem((ROWS, W), F32),
            vmem((1, T), F32),
            vmem((NV, 8, 128), F32),
            vmem((2, 8, 128), F32),
            vmem((Z, 8, 128), F32),
            dma((2 * NB + Z,)),
            dma((2, NE)), dma((2, NE)),
            dma((2, NE)), dma((2, NE)),
            dma((2,)),
            dma((2, NE)), dma((2, NE)),
            dma((2, NC)), dma((2, NC)),
            dma((NV,)), dma((NV,)),
            dma((NV,)), dma((NV,)),
            dma((NV,)), dma((NV,)),
            dma((NV,)), dma((NV,)),
            dma((Z,)), dma((Z,)),
            dma((2,)),
        ],
        compiler_params=pltpu.CompilerParams(
            collective_id=0, has_side_effects=True, vmem_limit_bytes=63 * 1024 * 1024
        ),
        name="step",
    )(hidden, head, target, ids.reshape(1, T))
    return loss[0, 0], gh.T, gw


def solution(mesh):
    sizes = mesh.shape
    tok, voc = sizes["tok"], sizes["voc"]
    side = {16: 4, 8: 4, 4: 2}[voc]
    Z, X, Y = tok // 2, side, voc // side
    torus = Mesh(mesh.devices.reshape(Z, 2, X, Y), TOK + VOC)

    def whole(hidden, head, target, ids):
        dims = (Z, X, Y, hidden.shape[0] // tok, hidden.shape[1], head.shape[1] // voc, 4)
        return jax.shard_map(
            functools.partial(body, dims),
            mesh=torus,
            in_specs=(P(TOK, None), P(TOK, VOC), P(TOK, VOC), P(TOK)),
            out_specs=(P(), P(TOK, VOC), P(TOK, VOC)),
            check_vma=False,
        )(hidden, head, target, ids)

    return whole
```

```python
import functools

import jax
import jax.numpy as jnp
from jax import lax
from jax.experimental import pallas as pl
from jax.experimental.pallas import tpu as pltpu
from jax.sharding import Mesh
from jax.sharding import PartitionSpec as P

VOC = ("voc_0", "voc_1")
TOK = ("tok_0", "tok_1")
CE = 0.5
F32 = jnp.float32
BF16 = jnp.bfloat16
MESH = pl.DeviceIdType.MESH
ROWS = 32
LOW = -1e30


def kernel(dims, *refs):
    Z, X, Y, T, D, V, NS = dims
    NV = X * Y
    NB = 2 * NS
    W = V // NB
    RB = D // (2 * Z)
    G = W // 128
    NE = (Z - 1) * NS
    NC = Z * NS
    NA = NS // 2
    NG = (Z - 2) * NA
    (
        hid_hbm, head_hbm, tgt_hbm, ids_hbm,
        loss_out, gh_out, gw_out,
        ids_ref, hg, hid, hid_t, tgt, zed, base, slope,
        part, sib_out, sib_in, ring_out, ring_in, gh_send, gh_recv,
        gh_acc, st_t, st_z, run_m, run_s, ids_c, m_c, s_c, own_t, lsum, row_t,
        l_xy, l_sib, l_z,
        in_sem, ready, ag_s, ag_r, al_s, al_r, sb_s, sb_r, sl_s, sl_r, so_sem,
        rs_s, rs_r, rb_s, rb_r, gh_s, gh_r, tt_s, tt_r, zz_s, zz_r,
        lx_s, lx_r, lz_s, lz_r, lb_sem,
    ) = refs
    z = lax.axis_index("tok_0")
    c = lax.axis_index("tok_1")
    x = lax.axis_index("voc_0")
    y = lax.axis_index("voc_1")
    me = x * Y + y
    sib = 1 - c
    right = lax.rem(z + 1, Z)
    left = lax.rem(z + Z - 1, Z)
    toward = ({"tok_0": right}, {"tok_0": left})
    other = {"tok_1": sib}

    def plane(k):
        j = lax.rem(me + k, NV)
        return j, {"voc_0": j // Y, "voc_1": lax.rem(j, Y)}

    def remote(src, dst, s, r, device):
        return pltpu.make_async_remote_copy(
            src_ref=src, dst_ref=dst, send_sem=s, recv_sem=r, device_id=device, device_id_type=MESH
        )

    mine = 2 * z + c

    def in_head(b):
        return pltpu.make_async_copy(head_hbm.at[:, pl.ds(b * W, W)], hg.at[mine, b], in_sem.at[b])

    def in_hid(k):
        return pltpu.make_async_copy(
            hid_hbm.at[:, pl.ds(k * 2 * RB, 2 * RB)], hid.at[k], in_sem.at[NB + k]
        )

    def in_tgt(b):
        return pltpu.make_async_copy(
            tgt_hbm.at[:, pl.ds(b * W, W)], tgt.at[b], in_sem.at[NB + Z + b]
        )

    in_ids = pltpu.make_async_copy(ids_hbm, ids_ref, in_sem.at[2 * NB + Z])
    for i in range(NS):
        for way in range(2):
            in_head(way * NS + i).start()
    in_ids.start()
    for k in range(Z):
        in_hid(k).start()
    for b in range(NB):
        in_tgt(b).start()

    barrier = pltpu.get_barrier_semaphore()
    row = [{"voc_0": lax.rem(x + k, X)} for k in range(1, X)]
    line = [{"voc_1": lax.rem(y + k, Y)} for k in range(1, Y)]
    near = (*toward, other, *row, *line)
    for device in near:
        pl.semaphore_signal(barrier, inc=1, device_id=device, device_id_type=MESH)
    pl.semaphore_wait(barrier, len(near))

    def chip_at(way, s):
        return lax.rem(z + Z - s, Z) if way == 0 else lax.rem(z + s, Z)

    def pair(way, n, s, core):
        return hg.at[2 * chip_at(way, s) + core, pl.ds(way * NS + 2 * lax.rem(n, NA), 2)]

    def ag(way, n, s):
        slot = pair(way, n, s, c)
        return remote(slot, slot, ag_s.at[way, n], ag_r.at[way, n], toward[way])

    def sb(way, n, core):
        slot = pair(way, n, n // NA + 1, core)
        return remote(slot, slot, sb_s.at[way, n], sb_r.at[way, n], other)

    def al(way, i, s):
        slot = hg.at[2 * chip_at(way, s) + c, way * NS + i]
        return remote(slot, slot, al_s.at[way, i], al_r.at[way, i], toward[way])

    def sl(way, i, core):
        slot = hg.at[2 * chip_at(way, Z - 1) + core, way * NS + i]
        return remote(slot, slot, sl_s.at[way, i], sl_r.at[way, i], other)

    def shard(core):
        slot = hg.at[2 * z + core]
        return remote(slot, slot, so_sem.at[0], so_sem.at[1], other)

    for i in range(NA):
        for way in range(2):
            for e in range(2):
                in_head(way * NS + 2 * i + e).wait()
            ag(way, i, 0).start()
    shard(c).start()
    for device in row:
        pl.semaphore_signal(ready, inc=1, device_id=device, device_id_type=MESH)

    @pl.loop(0, NB)
    def _(b):
        zed[b] = jnp.zeros((T, W), F32)

    @pl.loop(0, Z)
    def _(k):
        in_hid(k).wait()
        hid_t[k] = hid[k].T

    def column(row):
        return jnp.broadcast_to(row, (128, T)).T

    in_ids.wait()
    ids_c[...] = column(ids_ref[...].astype(F32))

    def reset():
        run_m[...] = jnp.full((T, 128), LOW, F32)
        run_s[...] = jnp.zeros((T, 128), F32)

    reset()
    own_t[...] = jnp.zeros((ROWS, W), F32)
    lsum[...] = jnp.zeros((ROWS, W), F32)

    def groups(v):
        return [v[:, g * 128 : (g + 1) * 128] for g in range(G)]

    def stats(load):
        @pl.loop(0, T // ROWS)
        def _(k):
            at = pl.ds(pl.multiple_of(k * ROWS, ROWS), ROWS)
            cols = groups(load(at))
            old = run_m[at]
            new = functools.reduce(jnp.maximum, cols, old)
            total = run_s[at] * jnp.exp(old - new)
            run_s[at] = total + functools.reduce(jnp.add, [jnp.exp(v - new) for v in cols])
            run_m[at] = new

    def local_stats():
        m = run_m[...].T
        top = jnp.max(m, axis=0, keepdims=True)
        return top, jnp.sum(run_s[...].T * jnp.exp(m - top), axis=0, keepdims=True)

    def st(ref, s, r, k):
        return remote(ref.at[me], ref.at[me], s.at[k], r.at[me], plane(k)[1])

    def st_in(ref, s, r, k):
        j, device = plane(k)
        return remote(ref.at[j], ref.at[j], s.at[k], r.at[j], device)

    def send_stats(ref, s, r):
        top, total = local_stats()
        ref[me] = jnp.concatenate([top, total], axis=0)
        for k in range(1, NV):
            st(ref, s, r, k).start()

    def joined_stats(ref, s, r):
        for k in range(1, NV):
            st_in(ref, s, r, k).wait_recv()
        all_m = jnp.concatenate([ref[j][0:1] for j in range(NV)], axis=0)
        all_s = jnp.concatenate([ref[j][1:2] for j in range(NV)], axis=0)
        top = jnp.max(all_m, axis=0, keepdims=True)
        return top, jnp.sum(all_s * jnp.exp(all_m - top), axis=0, keepdims=True)

    lane = lax.broadcasted_iota(jnp.int32, (ROWS, W), 1)

    def wide(v):
        return jnp.concatenate([v] * G, axis=1)

    def fill_base(b):
        col = (lane + (me * V + b * W)).astype(F32)

        @pl.loop(0, T // ROWS)
        def _(k):
            at = pl.ds(pl.multiple_of(k * ROWS, ROWS), ROWS)
            t = tgt[b, at].astype(F32)
            p = jnp.exp(t - wide(m_c[at])) * wide(s_c[at])
            own = col == wide(ids_c[at])
            base[b, at] = jnp.where(own, p + CE, p)
            own_t[...] += jnp.where(own, t, 0.0)

    def draft(s, b, way):
        chips = (chip_at(way, s - 1), chip_at(way, s))
        lhs = jnp.concatenate([hid[k] for k in chips], axis=1)
        rhs = jnp.concatenate([hg[2 * k + e, b] for k in chips for e in range(2)], axis=0)
        zed[b] += jnp.dot(lhs, rhs, preferred_element_type=F32)

    for b in range(NB):
        in_tgt(b).wait()
    shard(sib).wait_recv()

    @pl.loop(0, NG + 1)
    def _(n):
        s = n // NA + 1
        i = lax.rem(n, NA)

        @pl.when(n < NG)
        def _():
            for way in range(2):
                ag(way, n, s).wait_recv()

                @pl.when(n + NA < NG)
                def _():
                    ag(way, n + NA, s).start()

                @pl.when(n + NA >= NG)
                def _():
                    for e in range(2):
                        al(way, 2 * i + e, s).start()

                sb(way, n, c).start()

        @pl.when(n > 0)
        def _():
            m = n - 1
            for way in range(2):
                sb(way, m, sib).wait_recv()

            @pl.when(lax.rem(m // NA, 2) == 0)
            def _():
                @pl.loop(0, 2)
                def _(e):
                    for way in range(2):
                        draft(m // NA + 1, way * NS + 2 * lax.rem(m, NA) + e, way)

        @pl.when(s == 2)
        def _():
            @pl.loop(0, 2)
            def _(e):
                for way in range(2):
                    stats(lambda at: tgt[way * NS + 2 * i + e, at].astype(F32))

        @pl.when((s == 3) & (i == 0))
        def _():
            pl.semaphore_wait(ready, X - 1)
            send_stats(st_t, tt_s, tt_r)
            reset()

        @pl.when((s == 4) & (i == NA - 1))
        def _():
            top, total = joined_stats(st_t, tt_s, tt_r)
            m_c[...] = column(top)
            s_c[...] = column(1.0 / total)
            row_t[...] = top + jnp.log(total)

        @pl.when(s == Z - 2)
        def _():
            @pl.loop(0, 2)
            def _(e):
                for way in range(2):
                    fill_base(way * NS + 2 * i + e)

    @pl.loop(0, NS + 1)
    def _(i):
        @pl.when(i < NS)
        def _():
            for way in range(2):
                al(way, i, Z - 1).wait_recv()
                sl(way, i, c).start()

        @pl.when(i > 0)
        def _():
            for way in range(2):
                sl(way, i - 1, sib).wait_recv()
            for way in range(2):
                b = way * NS + i - 1
                draft(Z - 1, b, way)
                stats(lambda at: zed[b, at])

    send_stats(st_z, zz_s, zz_r)
    top_z, total_z = joined_stats(st_z, zz_s, zz_r)
    m_c[...] = column(top_z)
    s_c[...] = column((1.0 + CE) / total_z)
    row_t[...] = ((1.0 + CE) * (top_z + jnp.log(total_z)) - row_t[...]) * (1.0 / NV)

    def fill_slope(b):
        @pl.loop(0, T // ROWS)
        def _(k):
            at = pl.ds(pl.multiple_of(k * ROWS, ROWS), ROWS)
            q = jnp.exp(zed[b, at] - wide(m_c[at])) * wide(s_c[at])
            slope[b, at] = (q - base[b, at]).astype(BF16)

    def rb(way, n):
        return remote(
            sib_out.at[way, n], sib_in.at[way, n], rb_s.at[way, n], rb_r.at[way, n], other
        )

    def rs(way, n):
        return remote(
            ring_out.at[way, n], ring_in.at[way, n], rs_s.at[way, n], rs_r.at[way, n], toward[way]
        )

    def compute(n):
        s = n // NS
        slot = lax.rem(n, 2)
        for way in range(2):
            b = way * NS + lax.rem(n, NS)
            got = jnp.dot(hid_t[chip_at(way, s + 1)], slope[b], preferred_element_type=F32)
            part[slot, way, 0] = got[:RB]
            part[slot, way, 1] = got[RB:]
            sib_out[way, n] = part[slot, way, sib].astype(BF16)
            rb(way, n).start()

    def finish(n):
        s = n // NS
        slot = lax.rem(n, 2)
        for way in range(2):
            rb(way, n).wait_recv()

            @pl.when(s == 0)
            def _():
                val = part[slot, way, c] + sib_in[way, n].astype(F32)
                ring_out[way, n] = val.astype(BF16)
                rs(way, n).start()

            @pl.when(s > 0)
            def _():
                rs(way, n - NS).wait_recv()
                val = (part[slot, way, c] + sib_in[way, n].astype(F32)) + ring_in[
                    way, n - NS
                ].astype(F32)

                @pl.when(s < Z - 1)
                def _():
                    ring_out[way, n] = val.astype(BF16)
                    rs(way, n).start()

                @pl.when(s == Z - 1)
                def _():
                    b = way * NS + lax.rem(n, NS)
                    gw_out[:, pl.ds(pl.multiple_of(b * W, W), W)] = val

    def gh(j):
        device = {"voc_0": j // Y, "voc_1": lax.rem(j, Y)}
        return remote(gh_send.at[j], gh_recv.at[me], gh_s.at[j], gh_r.at[me], device)

    def gh_in(k):
        j, device = plane(k)
        return remote(gh_send.at[j], gh_recv.at[j], gh_s.at[j], gh_r.at[j], device)

    def hidden_part(e):
        r = lax.rem(e // 4 + me // 4, NV // 4)
        q = lax.rem(e, 4)
        got = []
        for k in range(NB // 4):
            b = q * (NB // 4) + k
            lhs = jnp.concatenate([hg[4 * r + i, b] for i in range(4)], axis=0)
            got.append(
                lax.dot_general(
                    lhs, slope[b], (((1,), (1,)), ((), ())), preferred_element_type=F32
                )
            )
        got = functools.reduce(jnp.add, got)

        @pl.when(q == 0)
        def _():
            gh_acc[...] = got

        @pl.when(q > 0)
        def _():
            gh_acc[...] += got

        @pl.when(q == 3)
        def _():
            for i in range(4):
                gh_send[4 * r + i] = gh_acc[i * RB : (i + 1) * RB].astype(BF16)

                @pl.when(4 * r + i != me)
                def _():
                    gh(4 * r + i).start()

    def loss_part(b):
        @pl.loop(0, T // ROWS)
        def _(k):
            at = pl.ds(pl.multiple_of(k * ROWS, ROWS), ROWS)
            lsum[...] += base[b, at] * (tgt[b, at].astype(F32) - zed[b, at])

    def total_of(v):
        return jnp.sum(jnp.sum(v, axis=0, keepdims=True), axis=1, keepdims=True)

    def sib_loss():
        return remote(l_sib.at[0], l_sib.at[1], lb_sem.at[0], lb_sem.at[1], other)

    def ring_loss(k):
        slot = l_z.at[chip_at(0, k)]
        return remote(slot, slot, lz_s.at[k], lz_r.at[k], toward[0])

    def ring_loss_in(k):
        slot = l_z.at[chip_at(0, k + 1)]
        return remote(slot, slot, lz_s.at[k], lz_r.at[k], toward[0])

    @pl.loop(0, NC + 1)
    def _(n):
        @pl.when(n < NS)
        def _():
            for way in range(2):
                fill_slope(way * NS + n)

        @pl.when(n < NC)
        def _():
            compute(n)

        @pl.when(n > 0)
        def _():
            finish(n - 1)

        @pl.when((n >= 2 * NS) & (n < 2 * NS + NV))
        def _():
            hidden_part(n - 2 * NS)

        @pl.when((n >= NS) & (n < 2 * NS))
        def _():
            for way in range(2):
                loss_part(way * NS + lax.rem(n, NS))

        @pl.when(n == 2 * NS)
        def _():
            local = total_of(lsum[...] - CE * own_t[...]) + total_of(row_t[...])
            l_xy[me] = jnp.broadcast_to(local, (8, 128))
            for k in range(1, NV):
                st(l_xy, lx_s, lx_r, k).start()

        @pl.when(n == 3 * NS - 1)
        def _():
            for k in range(1, NV):
                st_in(l_xy, lx_s, lx_r, k).wait_recv()
            l_sib[0] = functools.reduce(jnp.add, [l_xy[j] for j in range(NV)])
            sib_loss().start()

        @pl.when(n == 3 * NS)
        def _():
            sib_loss().wait_recv()
            l_z[z] = l_sib[0] + l_sib[1]
            ring_loss(0).start()

        @pl.when((n > 3 * NS) & (n <= 3 * NS + 2 * (Z - 1)) & (lax.rem(n - 3 * NS, 2) == 0))
        def _():
            k = (n - 3 * NS) // 2
            ring_loss_in(k - 1).wait_recv()

            @pl.when(k < Z - 1)
            def _():
                ring_loss(k).start()

    loss_out[...] = functools.reduce(jnp.add, [l_z[k] for k in range(Z)]) * (1.0 / (2 * Z * T))
    for k in range(1, NV):
        gh_in(k).wait_recv()
    gh_recv[me] = gh_send[me]
    gh_out[...] = functools.reduce(jnp.add, [gh_recv[j].astype(F32) for j in range(NV)])

    shard(c).wait_send()
    sib_loss().wait_send()

    @pl.loop(0, NG)
    def _(n):
        for way in range(2):
            ag(way, n, 0).wait_send()
            sb(way, n, c).wait_send()

    @pl.loop(0, NS)
    def _(i):
        for way in range(2):
            al(way, i, 0).wait_send()
            sl(way, i, c).wait_send()

    @pl.loop(0, NE)
    def _(n):
        for way in range(2):
            rs(way, n).wait_send()

    @pl.loop(0, NC)
    def _(n):
        for way in range(2):
            rb(way, n).wait_send()

    @pl.loop(0, Z - 1)
    def _(k):
        ring_loss(k).wait_send()

    for k in range(1, NV):
        st(st_t, tt_s, tt_r, k).wait_send()
        st(st_z, zz_s, zz_r, k).wait_send()
        st(l_xy, lx_s, lx_r, k).wait_send()
        gh_in(k).wait_send()


def hand_over(loss, gh, gw, loss_out, gh_out, gw_out, sems):
    copies = [
        pltpu.make_async_copy(src, dst, sems.at[k])
        for k, (src, dst) in enumerate(((gw, gw_out), (gh, gh_out)))
    ]
    for copy in copies:
        copy.start()
    loss_out[...] = loss[0:1, 0:1]
    for copy in copies:
        copy.wait()


def body(dims, hidden, head, target, ids):
    Z, X, Y, T, D, V, NS = dims
    NV = X * Y
    NB = 2 * NS
    W = V // NB
    RB = D // (2 * Z)
    NE, NC, NG = (Z - 1) * NS, Z * NS, (Z - 2) * NS // 2
    vmem, dma = pltpu.VMEM, pltpu.SemaphoreType.DMA
    hbm = pl.BlockSpec(memory_space=pltpu.HBM)
    local = pl.BlockSpec(memory_space=pltpu.VMEM)
    loss, gh, gw = pl.pallas_call(
        functools.partial(kernel, dims),
        out_shape=(
            vmem((8, 128), F32),
            vmem((RB, T), F32),
            vmem((RB, V), F32),
        ),
        in_specs=[hbm, hbm, hbm, hbm],
        out_specs=(local, local, local),
        scratch_shapes=[
            vmem((1, T), jnp.int32),
            vmem((2 * Z, NB, RB, W), BF16),
            vmem((Z, T, 2 * RB), BF16),
            vmem((Z, 2 * RB, T), BF16),
            vmem((NB, T, W), BF16),
            vmem((NB, T, W), F32),
            vmem((NB, T, W), F32),
            vmem((NB, T, W), BF16),
            vmem((2, 2, 2, RB, W), F32),
            vmem((2, NC, RB, W), BF16),
            vmem((2, NC, RB, W), BF16),
            vmem((2, NE, RB, W), BF16),
            vmem((2, NE, RB, W), BF16),
            vmem((NV, RB, T), BF16),
            vmem((NV, RB, T), BF16),
            vmem((4 * RB, T), F32),
            vmem((NV, 2, T), F32),
            vmem((NV, 2, T), F32),
            vmem((T, 128), F32),
            vmem((T, 128), F32),
            vmem((T, 128), F32),
            vmem((T, 128), F32),
            vmem((T, 128), F32),
            vmem((ROWS, W), F32),
            vmem((ROWS, W), F32),
            vmem((1, T), F32),
            vmem((NV, 8, 128), F32),
            vmem((2, 8, 128), F32),
            vmem((Z, 8, 128), F32),
            dma((2 * NB + Z + 1,)),
            pltpu.SemaphoreType.REGULAR,
            dma((2, NG)), dma((2, NG)),
            dma((2, NS)), dma((2, NS)),
            dma((2, NG)), dma((2, NG)),
            dma((2, NS)), dma((2, NS)),
            dma((2,)),
            dma((2, NE)), dma((2, NE)),
            dma((2, NC)), dma((2, NC)),
            dma((NV,)), dma((NV,)),
            dma((NV,)), dma((NV,)),
            dma((NV,)), dma((NV,)),
            dma((NV,)), dma((NV,)),
            dma((Z,)), dma((Z,)),
            dma((2,)),
        ],
        compiler_params=pltpu.CompilerParams(
            collective_id=0, has_side_effects=True, vmem_limit_bytes=58 * 1024 * 1024
        ),
        name="step",
    )(hidden, head, target, ids.reshape(1, T))
    loss, gh, gw = pl.pallas_call(
        hand_over,
        out_shape=(
            jax.ShapeDtypeStruct((1, 1), F32),
            jax.ShapeDtypeStruct((RB, T), F32),
            jax.ShapeDtypeStruct((RB, V), F32),
        ),
        in_specs=[local] * 3,
        out_specs=(local, hbm, hbm),
        scratch_shapes=[dma((3,))],
        compiler_params=pltpu.CompilerParams(vmem_limit_bytes=4 * 1024 * 1024),
        name="hand_over",
    )(loss, gh, gw)
    return loss.reshape(()), gh.T, gw


def solution(mesh):
    sizes = mesh.shape
    tok, voc = sizes["tok"], sizes["voc"]
    side = {16: 4, 8: 4, 4: 2}[voc]
    Z, X, Y = tok // 2, side, voc // side
    torus = Mesh(mesh.devices.reshape(Z, 2, X, Y), TOK + VOC)

    def whole(hidden, head, target, ids):
        dims = (Z, X, Y, hidden.shape[0] // tok, hidden.shape[1], head.shape[1] // voc, 4)
        return jax.shard_map(
            functools.partial(body, dims),
            mesh=torus,
            in_specs=(P(TOK, None), P(TOK, VOC), P(TOK, VOC), P(TOK)),
            out_specs=(P(), P(TOK, VOC), P(TOK, VOC)),
            check_vma=False,
        )(hidden, head, target, ids)

    return whole
```

```python
import functools

import jax
import jax.numpy as jnp
from jax import lax
from jax.experimental import pallas as pl
from jax.experimental.pallas import tpu as pltpu
from jax.sharding import Mesh
from jax.sharding import PartitionSpec as P

VOC = ("voc_0", "voc_1")
TOK = ("tok_0", "tok_1")
CE = 0.5
F32 = jnp.float32
BF16 = jnp.bfloat16
MESH = pl.DeviceIdType.MESH
ROWS = 32
UNROLL = 4
LOW = -1e30


def kernel(dims, *refs):
    Z, X, Y, T, D, V, NS = dims
    NV = X * Y
    NB = 2 * NS
    W = V // NB
    RB = D // (2 * Z)
    G = W // 128
    NA = NS // 2
    NG = (Z - 2) * NA
    NC = Z * NA
    (
        hid_hbm, head_hbm, tgt_hbm, ids_hbm,
        loss_out, gh_out, gw_out,
        ids_ref, hg, hid, hid_t, tgt, zed, base, slope,
        part, sib_out, sib_in, ring_out, ring_in, gh_send, gh_recv,
        gh_acc, st_t, st_z, run_m, run_s, ids_c, m_c, s_c, own_t, lsum, row_t,
        l_xy, l_sib, l_z,
        in_sem, ready, ag_s, ag_r, al_s, al_r, sb_s, sb_r, sl_s, sl_r, so_sem,
        rl_s, rl_r, rs_s, rs_r, bl_s, bl_r, rb_s, rb_r, gh_s, gh_r, tt_s, tt_r, zz_s, zz_r,
        lx_s, lx_r, lz_s, lz_r, lb_sem,
    ) = refs
    z = lax.axis_index("tok_0")
    c = lax.axis_index("tok_1")
    x = lax.axis_index("voc_0")
    y = lax.axis_index("voc_1")
    me = x * Y + y
    sib = 1 - c
    right = lax.rem(z + 1, Z)
    left = lax.rem(z + Z - 1, Z)
    toward = ({"tok_0": right}, {"tok_0": left})
    other = {"tok_1": sib}

    def plane(k):
        j = lax.rem(me + k, NV)
        return j, {"voc_0": j // Y, "voc_1": lax.rem(j, Y)}

    def remote(src, dst, s, r, device):
        return pltpu.make_async_remote_copy(
            src_ref=src, dst_ref=dst, send_sem=s, recv_sem=r, device_id=device, device_id_type=MESH
        )

    mine = 2 * z + c

    def in_head(b):
        return pltpu.make_async_copy(head_hbm.at[:, pl.ds(b * W, W)], hg.at[mine, b], in_sem.at[b])

    def in_hid(k):
        return pltpu.make_async_copy(
            hid_hbm.at[:, pl.ds(k * 2 * RB, 2 * RB)], hid.at[k], in_sem.at[NB + k]
        )

    def in_tgt(b):
        return pltpu.make_async_copy(
            tgt_hbm.at[:, pl.ds(b * W, W)], tgt.at[b], in_sem.at[NB + Z + b]
        )

    in_ids = pltpu.make_async_copy(ids_hbm, ids_ref, in_sem.at[2 * NB + Z])
    for i in range(NS):
        for way in range(2):
            in_head(way * NS + i).start()
    in_ids.start()
    for k in range(Z):
        in_hid(k).start()
    for b in range(NB):
        in_tgt(b).start()

    barrier = pltpu.get_barrier_semaphore()
    row = [{"voc_0": lax.rem(x + k, X)} for k in range(1, X)]
    line = [{"voc_1": lax.rem(y + k, Y)} for k in range(1, Y)]
    near = (*toward, other, *row, *line)
    for device in near:
        pl.semaphore_signal(barrier, inc=1, device_id=device, device_id_type=MESH)
    pl.semaphore_wait(barrier, len(near))

    def chip_at(way, s):
        return lax.rem(z + Z - s, Z) if way == 0 else lax.rem(z + s, Z)

    def pair(way, n, s, core):
        return hg.at[2 * chip_at(way, s) + core, pl.ds(way * NS + 2 * lax.rem(n, NA), 2)]

    def ag(way, n, s):
        slot = pair(way, n, s, c)
        return remote(slot, slot, ag_s.at[way, n], ag_r.at[way, n], toward[way])

    def sb(way, n, core):
        slot = pair(way, n, n // NA + 1, core)
        return remote(slot, slot, sb_s.at[way, n], sb_r.at[way, n], other)

    def al(way, i, s):
        slot = hg.at[2 * chip_at(way, s) + c, way * NS + i]
        return remote(slot, slot, al_s.at[way, i], al_r.at[way, i], toward[way])

    def sl(way, i, core):
        slot = hg.at[2 * chip_at(way, Z - 1) + core, way * NS + i]
        return remote(slot, slot, sl_s.at[way, i], sl_r.at[way, i], other)

    def shard(core):
        slot = hg.at[2 * z + core]
        return remote(slot, slot, so_sem.at[0], so_sem.at[1], other)

    for i in range(NA):
        for way in range(2):
            for e in range(2):
                in_head(way * NS + 2 * i + e).wait()
            ag(way, i, 0).start()
    shard(c).start()
    for device in row:
        pl.semaphore_signal(ready, inc=1, device_id=device, device_id_type=MESH)

    @pl.loop(0, NB)
    def _(b):
        zed[b] = jnp.zeros((T, W), F32)

    @pl.loop(0, Z)
    def _(k):
        in_hid(k).wait()
        hid_t[k] = hid[k].T

    def column(row):
        return jnp.broadcast_to(row, (128, T)).T

    in_ids.wait()
    ids_c[...] = column(ids_ref[...].astype(F32))

    def reset():
        run_m[...] = jnp.full((T, 128), LOW, F32)
        run_s[...] = jnp.zeros((T, 128), F32)

    reset()
    own_t[...] = jnp.zeros((ROWS, W), F32)
    lsum[...] = jnp.zeros((ROWS, W), F32)

    def groups(v):
        return [v[:, g * 128 : (g + 1) * 128] for g in range(G)]

    def rowwise(step):
        @pl.loop(0, T // (ROWS * UNROLL))
        def _(k):
            for u in range(UNROLL):
                step(pl.ds(pl.multiple_of((k * UNROLL + u) * ROWS, ROWS), ROWS))

    def stats(load):
        @rowwise
        def _(at):
            cols = groups(load(at))
            old = run_m[at]
            new = functools.reduce(jnp.maximum, cols, old)
            total = run_s[at] * jnp.exp(old - new)
            run_s[at] = total + functools.reduce(jnp.add, [jnp.exp(v - new) for v in cols])
            run_m[at] = new

    def local_stats():
        m = run_m[...].T
        top = jnp.max(m, axis=0, keepdims=True)
        return top, jnp.sum(run_s[...].T * jnp.exp(m - top), axis=0, keepdims=True)

    def st(ref, s, r, k):
        return remote(ref.at[me], ref.at[me], s.at[k], r.at[me], plane(k)[1])

    def st_in(ref, s, r, k):
        j, device = plane(k)
        return remote(ref.at[j], ref.at[j], s.at[k], r.at[j], device)

    def send_stats(ref, s, r):
        top, total = local_stats()
        ref[me] = jnp.concatenate([top, total], axis=0)
        for k in range(1, NV):
            st(ref, s, r, k).start()

    def joined_stats(ref, s, r):
        for k in range(1, NV):
            st_in(ref, s, r, k).wait_recv()
        rows = [ref[j] for j in range(NV)]
        top = functools.reduce(jnp.maximum, [v[0:1] for v in rows])
        return top, functools.reduce(jnp.add, [v[1:2] * jnp.exp(v[0:1] - top) for v in rows])

    lane = lax.broadcasted_iota(jnp.int32, (ROWS, W), 1)

    def wide(v):
        return jnp.concatenate([v] * G, axis=1)

    def fill_base(b):
        col = (lane + (me * V + b * W)).astype(F32)

        @rowwise
        def _(at):
            t = tgt[b, at].astype(F32)
            p = jnp.exp(t - wide(m_c[at])) * wide(s_c[at])
            own = col == wide(ids_c[at])
            base[b, at] = jnp.where(own, p + CE, p)
            own_t[...] += jnp.where(own, t, 0.0)

    def draft(s, b, way):
        chips = (chip_at(way, s - 1), chip_at(way, s))
        lhs = jnp.concatenate([hid[k] for k in chips], axis=1)
        rhs = jnp.concatenate([hg[2 * k + e, b] for k in chips for e in range(2)], axis=0)
        zed[b] += jnp.dot(lhs, rhs, preferred_element_type=F32)

    for b in range(NB):
        in_tgt(b).wait()
    shard(sib).wait_recv()

    @pl.loop(0, NG + 1)
    def _(n):
        s = n // NA + 1
        i = lax.rem(n, NA)

        @pl.when(n < NG)
        def _():
            for way in range(2):
                ag(way, n, s).wait_recv()

                @pl.when(n + NA < NG)
                def _():
                    ag(way, n + NA, s).start()

                @pl.when(n + NA >= NG)
                def _():
                    for e in range(2):
                        al(way, 2 * i + e, s).start()

                sb(way, n, c).start()

        @pl.when(n > 0)
        def _():
            m = n - 1
            for way in range(2):
                sb(way, m, sib).wait_recv()

            @pl.when(lax.rem(m // NA, 2) == 0)
            def _():
                @pl.loop(0, 2)
                def _(e):
                    for way in range(2):
                        draft(m // NA + 1, way * NS + 2 * lax.rem(m, NA) + e, way)

        @pl.when(s == 2)
        def _():
            @pl.loop(0, 2)
            def _(e):
                for way in range(2):
                    stats(lambda at: tgt[way * NS + 2 * i + e, at].astype(F32))

        @pl.when((s == 3) & (i == 0))
        def _():
            pl.semaphore_wait(ready, X - 1)
            send_stats(st_t, tt_s, tt_r)
            reset()

        @pl.when((s == 4) & (i == NA - 1))
        def _():
            top, total = joined_stats(st_t, tt_s, tt_r)
            m_c[...] = column(top)
            s_c[...] = column(1.0 / total)
            row_t[...] = top + jnp.log(total)

        @pl.when(s == Z - 2)
        def _():
            @pl.loop(0, 2)
            def _(e):
                for way in range(2):
                    fill_base(way * NS + 2 * i + e)

    @pl.loop(0, NS + 1)
    def _(i):
        @pl.when(i < NS)
        def _():
            for way in range(2):
                al(way, i, Z - 1).wait_recv()
                sl(way, i, c).start()

        @pl.when(i > 0)
        def _():
            for way in range(2):
                sl(way, i - 1, sib).wait_recv()
            for way in range(2):
                b = way * NS + i - 1
                draft(Z - 1, b, way)
                stats(lambda at: zed[b, at])

    send_stats(st_z, zz_s, zz_r)
    top_z, total_z = joined_stats(st_z, zz_s, zz_r)
    m_c[...] = column(top_z)
    s_c[...] = column((1.0 + CE) / total_z)
    row_t[...] = ((1.0 + CE) * (top_z + jnp.log(total_z)) - row_t[...]) * (1.0 / NV)

    def fill_slope(b):
        @rowwise
        def _(at):
            q = jnp.exp(zed[b, at] - wide(m_c[at])) * wide(s_c[at])
            slope[b, at] = (q - base[b, at]).astype(BF16)

    def rl(way, i):
        return remote(
            ring_out.at[way, 0, i], ring_in.at[way, 0, i], rl_s.at[way, i], rl_r.at[way, i], toward[way]
        )

    def bl(way, i):
        return remote(
            sib_out.at[way, 0, i], sib_in.at[way, 0, i], bl_s.at[way, i], bl_r.at[way, i], other
        )

    def both(n):
        return n // NA, pl.ds(2 * lax.rem(n, NA), 2)

    def rs(way, n):
        at = both(n)
        return remote(
            ring_out.at[way, *at], ring_in.at[way, *at], rs_s.at[way, n], rs_r.at[way, n], toward[way]
        )

    def rb(way, n):
        at = both(n)
        return remote(
            sib_out.at[way, *at], sib_in.at[way, *at], rb_s.at[way, n], rb_r.at[way, n], other
        )

    def product(way, s, i, own):
        got = jnp.dot(
            hid_t[chip_at(way, s + 1)], slope[way * NS + i], preferred_element_type=F32
        )
        own[0] = got[:RB]
        own[1] = got[RB:]
        sib_out[way, s, i] = own[sib].astype(BF16)

    def compute(n):
        for way in range(2):
            for e in range(2):
                product(way, n // NA, 2 * lax.rem(n, NA) + e, part.at[lax.rem(n, 2), way, e])
            rb(way, n).start()

    def finish_first(i):
        for way in range(2):
            bl(way, i).wait_recv()
            val = part[lax.rem(i, 2), way, 0, c] + sib_in[way, 0, i].astype(F32)
            ring_out[way, 0, i] = val.astype(BF16)
            rl(way, i).start()

    def finish(n):
        s = n // NA
        for way in range(2):
            rb(way, n).wait_recv()

            @pl.when(s == 1)
            def _():
                for e in range(2):
                    rl(way, 2 * lax.rem(n, NA) + e).wait_recv()

            @pl.when(s > 1)
            def _():
                rs(way, n - NA).wait_recv()

            for e in range(2):
                i = 2 * lax.rem(n, NA) + e
                own = part[lax.rem(n, 2), way, e, c] + sib_in[way, s, i].astype(F32)
                val = own + ring_in[way, s - 1, i].astype(F32)

                @pl.when(s < Z - 1)
                def _():
                    ring_out[way, s, i] = val.astype(BF16)

                @pl.when(s == Z - 1)
                def _():
                    at = pl.ds(pl.multiple_of((way * NS + i) * W, W), W)
                    gw_out[:, at] = val

            @pl.when(s < Z - 1)
            def _():
                rs(way, n).start()

    def gh(j):
        device = {"voc_0": j // Y, "voc_1": lax.rem(j, Y)}
        return remote(gh_send.at[j], gh_recv.at[me], gh_s.at[j], gh_r.at[me], device)

    def gh_in(k):
        j, device = plane(k)
        return remote(gh_send.at[j], gh_recv.at[j], gh_s.at[j], gh_r.at[j], device)

    def hidden_part(e):
        r = lax.rem(e // 4 + me // 4, NV // 4)
        q = lax.rem(e, 4)
        got = []
        for k in range(NB // 4):
            b = q * (NB // 4) + k
            lhs = jnp.concatenate([hg[4 * r + i, b] for i in range(4)], axis=0)
            got.append(
                lax.dot_general(
                    lhs, slope[b], (((1,), (1,)), ((), ())), preferred_element_type=F32
                )
            )
        got = functools.reduce(jnp.add, got)

        @pl.when(q == 0)
        def _():
            gh_acc[...] = got

        @pl.when(q > 0)
        def _():
            gh_acc[...] += got

        @pl.when(q == 3)
        def _():
            for i in range(4):
                gh_send[4 * r + i] = gh_acc[i * RB : (i + 1) * RB].astype(BF16)

                @pl.when(4 * r + i != me)
                def _():
                    gh(4 * r + i).start()

    def loss_part(b):
        @rowwise
        def _(at):
            lsum[...] += base[b, at] * (tgt[b, at].astype(F32) - zed[b, at])

    def total_of(v):
        return jnp.sum(jnp.sum(v, axis=0, keepdims=True), axis=1, keepdims=True)

    def sib_loss():
        return remote(l_sib.at[0], l_sib.at[1], lb_sem.at[0], lb_sem.at[1], other)

    def ring_loss(k):
        slot = l_z.at[chip_at(0, k)]
        return remote(slot, slot, lz_s.at[k], lz_r.at[k], toward[0])

    def ring_loss_in(k):
        slot = l_z.at[chip_at(0, k + 1)]
        return remote(slot, slot, lz_s.at[k], lz_r.at[k], toward[0])

    def sent():
        shard(c).wait_send()

        @pl.loop(0, NG)
        def _(n):
            for way in range(2):
                ag(way, n, 0).wait_send()
                sb(way, n, c).wait_send()

        @pl.loop(0, NS)
        def _(i):
            for way in range(2):
                al(way, i, 0).wait_send()
                sl(way, i, c).wait_send()

        for k in range(1, NV):
            st(st_t, tt_s, tt_r, k).wait_send()
            st(st_z, zz_s, zz_r, k).wait_send()

    def gathered():
        loss_out[...] = functools.reduce(jnp.add, [l_z[k] for k in range(Z)]) * (
            1.0 / (2 * Z * T)
        )
        for k in range(1, NV):
            gh_in(k).wait_recv()
        gh_recv[me] = gh_send[me]

        @pl.loop(0, RB // 16)
        def _(k):
            at = pl.ds(pl.multiple_of(k * 16, 16), 16)
            gh_out[at] = functools.reduce(jnp.add, [gh_recv[j, at].astype(F32) for j in range(NV)])

        sib_loss().wait_send()

        @pl.loop(0, Z - 1)
        def _(k):
            ring_loss(k).wait_send()

        for k in range(1, NV):
            st(l_xy, lx_s, lx_r, k).wait_send()
            gh_in(k).wait_send()

    @pl.loop(0, NS)
    def _(i):
        for way in range(2):
            fill_slope(way * NS + i)
            product(way, 0, i, part.at[lax.rem(i, 2), way, 0])
            bl(way, i).start()

        @pl.when(i > 0)
        def _():
            finish_first(i - 1)

    @pl.loop(NA, NC + 1)
    def _(n):
        @pl.when(n < NC)
        def _():
            compute(n)

        @pl.when(n == NA)
        def _():
            finish_first(NS - 1)

        @pl.when(n > NA)
        def _():
            finish(n - 1)

        @pl.when(n == NA + 1)
        def _():
            sent()

        @pl.when((n > NA) & (n <= NA + 2))
        def _():
            @pl.loop(0, NB // 2)
            def _(k):
                loss_part((n - NA - 1) * (NB // 2) + k)

        @pl.when(n == NA + 3)
        def _():
            local = total_of(lsum[...] - CE * own_t[...]) + total_of(row_t[...])
            l_xy[me] = jnp.broadcast_to(local, (8, 128))
            for k in range(1, NV):
                st(l_xy, lx_s, lx_r, k).start()

        @pl.when((n >= NA + 3) & (n < NA + 3 + NV // 2))
        def _():
            @pl.loop(0, 2)
            def _(e):
                hidden_part(2 * (n - NA - 3) + e)

        @pl.when(n == NA + 4)
        def _():
            for k in range(1, NV):
                st_in(l_xy, lx_s, lx_r, k).wait_recv()
            l_sib[0] = functools.reduce(jnp.add, [l_xy[j] for j in range(NV)])
            sib_loss().start()

        @pl.when(n == NA + 5)
        def _():
            sib_loss().wait_recv()
            l_z[z] = l_sib[0] + l_sib[1]
            ring_loss(0).start()

        @pl.when((n > NA + 5) & (n <= NA + 5 + Z - 1))
        def _():
            k = n - NA - 5
            ring_loss_in(k - 1).wait_recv()

            @pl.when(k < Z - 1)
            def _():
                ring_loss(k).start()

        @pl.when(n == NC - 1)
        def _():
            gathered()

    @pl.loop(0, NS)
    def _(i):
        for way in range(2):
            rl(way, i).wait_send()
            bl(way, i).wait_send()

    @pl.loop(NA, NC - NA)
    def _(n):
        for way in range(2):
            rs(way, n).wait_send()

    @pl.loop(NA, NC)
    def _(n):
        for way in range(2):
            rb(way, n).wait_send()


def hand_over(loss, gh, gw, loss_out, gh_out, gw_out, sems):
    copies = [
        pltpu.make_async_copy(src, dst, sems.at[k])
        for k, (src, dst) in enumerate(((gw, gw_out), (gh, gh_out)))
    ]
    for copy in copies:
        copy.start()
    loss_out[...] = loss[0:1, 0:1]
    for copy in copies:
        copy.wait()


def body(dims, hidden, head, target, ids):
    Z, X, Y, T, D, V, NS = dims
    NV = X * Y
    NB = 2 * NS
    W = V // NB
    RB = D // (2 * Z)
    NA = NS // 2
    NC, NG = Z * NA, (Z - 2) * NA
    vmem, dma = pltpu.VMEM, pltpu.SemaphoreType.DMA
    hbm = pl.BlockSpec(memory_space=pltpu.HBM)
    local = pl.BlockSpec(memory_space=pltpu.VMEM)
    loss, gh, gw = pl.pallas_call(
        functools.partial(kernel, dims),
        out_shape=(
            vmem((8, 128), F32),
            vmem((RB, T), F32),
            vmem((RB, V), F32),
        ),
        in_specs=[hbm, hbm, hbm, hbm],
        out_specs=(local, local, local),
        scratch_shapes=[
            vmem((1, T), jnp.int32),
            vmem((2 * Z, NB, RB, W), BF16),
            vmem((Z, T, 2 * RB), BF16),
            vmem((Z, 2 * RB, T), BF16),
            vmem((NB, T, W), BF16),
            vmem((NB, T, W), F32),
            vmem((NB, T, W), F32),
            vmem((NB, T, W), BF16),
            vmem((2, 2, 2, 2, RB, W), F32),
            vmem((2, Z, NS, RB, W), BF16),
            vmem((2, Z, NS, RB, W), BF16),
            vmem((2, Z - 1, NS, RB, W), BF16),
            vmem((2, Z - 1, NS, RB, W), BF16),
            vmem((NV, RB, T), BF16),
            vmem((NV, RB, T), BF16),
            vmem((4 * RB, T), F32),
            vmem((NV, 2, T), F32),
            vmem((NV, 2, T), F32),
            vmem((T, 128), F32),
            vmem((T, 128), F32),
            vmem((T, 128), F32),
            vmem((T, 128), F32),
            vmem((T, 128), F32),
            vmem((ROWS, W), F32),
            vmem((ROWS, W), F32),
            vmem((1, T), F32),
            vmem((NV, 8, 128), F32),
            vmem((2, 8, 128), F32),
            vmem((Z, 8, 128), F32),
            dma((2 * NB + Z + 1,)),
            pltpu.SemaphoreType.REGULAR,
            dma((2, NG)), dma((2, NG)),
            dma((2, NS)), dma((2, NS)),
            dma((2, NG)), dma((2, NG)),
            dma((2, NS)), dma((2, NS)),
            dma((2,)),
            dma((2, NS)), dma((2, NS)),
            dma((2, NC)), dma((2, NC)),
            dma((2, NS)), dma((2, NS)),
            dma((2, NC)), dma((2, NC)),
            dma((NV,)), dma((NV,)),
            dma((NV,)), dma((NV,)),
            dma((NV,)), dma((NV,)),
            dma((NV,)), dma((NV,)),
            dma((Z,)), dma((Z,)),
            dma((2,)),
        ],
        compiler_params=pltpu.CompilerParams(
            collective_id=0, has_side_effects=True, vmem_limit_bytes=60 * 1024 * 1024
        ),
        name="step",
    )(hidden, head, target, ids.reshape(1, T))
    loss, gh, gw = pl.pallas_call(
        hand_over,
        out_shape=(
            jax.ShapeDtypeStruct((1, 1), F32),
            jax.ShapeDtypeStruct((RB, T), F32),
            jax.ShapeDtypeStruct((RB, V), F32),
        ),
        in_specs=[local] * 3,
        out_specs=(local, hbm, hbm),
        scratch_shapes=[dma((3,))],
        compiler_params=pltpu.CompilerParams(vmem_limit_bytes=4 * 1024 * 1024),
        name="hand_over",
    )(loss, gh, gw)
    return loss.reshape(()), gh.T, gw


def solution(mesh):
    sizes = mesh.shape
    tok, voc = sizes["tok"], sizes["voc"]
    side = {16: 4, 8: 4, 4: 2}[voc]
    Z, X, Y = tok // 2, side, voc // side
    torus = Mesh(mesh.devices.reshape(Z, 2, X, Y), TOK + VOC)

    def whole(hidden, head, target, ids):
        dims = (Z, X, Y, hidden.shape[0] // tok, hidden.shape[1], head.shape[1] // voc, 4)
        return jax.shard_map(
            functools.partial(body, dims),
            mesh=torus,
            in_specs=(P(TOK, None), P(TOK, VOC), P(TOK, VOC), P(TOK)),
            out_specs=(P(), P(TOK, VOC), P(TOK, VOC)),
            check_vma=False,
        )(hidden, head, target, ids)

    return whole
```

```python
import functools

import jax
import jax.numpy as jnp
from jax import lax
from jax.experimental import pallas as pl
from jax.experimental.pallas import tpu as pltpu
from jax.sharding import Mesh
from jax.sharding import PartitionSpec as P

VOC = ("voc_0", "voc_1")
TOK = ("tok_0", "tok_1")
CE = 0.5
F32 = jnp.float32
BF16 = jnp.bfloat16
MESH = pl.DeviceIdType.MESH
ROWS = 32
UNROLL = 8
LOW = -1e30


def kernel(dims, *refs):
    Z, X, Y, T, D, V, NS = dims
    NV = X * Y
    NB = 2 * NS
    W = V // NB
    RB = D // (2 * Z)
    G = W // 128
    NA = NS // 2
    NG = (Z - 2) * NA
    NC = Z * NA
    (
        hid_hbm, head_hbm, tgt_hbm, ids_hbm,
        loss_out, gh_out, gw_out,
        ids_ref, hg, hid, hid_t, tgt, zed, base, slope,
        part, sib_out, sib_in, ring_out, ring_in, gh_send, gh_recv,
        gh_acc, st_t, st_z, run_m, run_s, ids_c, m_c, s_c, own_t, lsum, row_t,
        l_xy, l_sib, l_z,
        in_sem, ready, ag_s, ag_r, al_s, al_r, sb_s, sb_r, sl_s, sl_r, so_sem,
        rl_s, rl_r, rs_s, rs_r, bl_s, bl_r, rb_s, rb_r, gh_s, gh_r, tt_s, tt_r, zz_s, zz_r,
        lx_s, lx_r, lz_s, lz_r, lb_sem,
    ) = refs
    z = lax.axis_index("tok_0")
    c = lax.axis_index("tok_1")
    x = lax.axis_index("voc_0")
    y = lax.axis_index("voc_1")
    me = x * Y + y
    sib = 1 - c
    right = lax.rem(z + 1, Z)
    left = lax.rem(z + Z - 1, Z)
    toward = ({"tok_0": right}, {"tok_0": left})
    other = {"tok_1": sib}

    steps = [(dx, dy) for dx in range(X) for dy in range(Y) if dx or dy]
    steps.sort(key=lambda d: -min(d[0], X - d[0]) - min(d[1], Y - d[1]))

    def plane(k):
        px, py = lax.rem(x + steps[k - 1][0], X), lax.rem(y + steps[k - 1][1], Y)
        return px * Y + py, {"voc_0": px, "voc_1": py}

    def remote(src, dst, s, r, device):
        return pltpu.make_async_remote_copy(
            src_ref=src, dst_ref=dst, send_sem=s, recv_sem=r, device_id=device, device_id_type=MESH
        )

    mine = 2 * z + c

    def in_head(b):
        return pltpu.make_async_copy(head_hbm.at[:, pl.ds(b * W, W)], hg.at[mine, b], in_sem.at[b])

    def in_hid(k):
        return pltpu.make_async_copy(
            hid_hbm.at[:, pl.ds(k * 2 * RB, 2 * RB)], hid.at[k], in_sem.at[NB + k]
        )

    def in_tgt(b):
        return pltpu.make_async_copy(
            tgt_hbm.at[:, pl.ds(b * W, W)], tgt.at[b], in_sem.at[NB + Z + b]
        )

    in_ids = pltpu.make_async_copy(ids_hbm, ids_ref, in_sem.at[2 * NB + Z])
    for i in range(NS):
        for way in range(2):
            in_head(way * NS + i).start()
    in_ids.start()

    barrier = pltpu.get_barrier_semaphore()
    def tell(sem, device):
        pl.semaphore_signal(sem, inc=1, device_id=device, device_id_type=MESH)

    below_x, below_y = {"voc_0": x - 1}, {"voc_1": y - 1}
    for device in (*toward, other):
        tell(barrier, device)

    @pl.when(x < X - 1)
    def _():
        tell(barrier, {"voc_0": x + 1})

    @pl.when((x == 0) & (y < Y - 1))
    def _():
        tell(barrier, {"voc_1": y + 1})

    pl.semaphore_wait(barrier, 3 + jnp.where((x > 0) | (y > 0), 1, 0))

    def word(n):
        @pl.when((x > 0) & (n == X - 1 - x))
        def _():
            @pl.when(x < X - 1)
            def _():
                pl.semaphore_wait(ready.at[0], 1)

            tell(ready.at[0], below_x)

        @pl.when((x == 0) & (n == X - 1))
        def _():
            pl.semaphore_wait(ready.at[0], 1)

        @pl.when((x == 0) & (y > 0) & (n == X - 1 + Y - 1 - y))
        def _():
            @pl.when(y < Y - 1)
            def _():
                pl.semaphore_wait(ready.at[1], 1)

            tell(ready.at[1], below_y)

        @pl.when((me == 0) & (n == X - 1 + Y - 1))
        def _():
            pl.semaphore_wait(ready.at[1], 1)
            for k in range(1, NV):
                tell(ready.at[2], plane(k)[1])

    def chip_at(way, s):
        return lax.rem(z + Z - s, Z) if way == 0 else lax.rem(z + s, Z)

    def pair(way, n, s, core):
        return hg.at[2 * chip_at(way, s) + core, pl.ds(way * NS + 2 * lax.rem(n, NA), 2)]

    def ag(way, n, s):
        slot = pair(way, n, s, c)
        return remote(slot, slot, ag_s.at[way, n], ag_r.at[way, n], toward[way])

    def sb(way, n, core):
        slot = pair(way, n, n // NA + 1, core)
        return remote(slot, slot, sb_s.at[way, n], sb_r.at[way, n], other)

    def al(way, i, s):
        slot = hg.at[2 * chip_at(way, s) + c, way * NS + i]
        return remote(slot, slot, al_s.at[way, i], al_r.at[way, i], toward[way])

    def sl(way, i, core):
        slot = hg.at[2 * chip_at(way, Z - 1) + core, way * NS + i]
        return remote(slot, slot, sl_s.at[way, i], sl_r.at[way, i], other)

    def shard(core):
        slot = hg.at[2 * z + core]
        return remote(slot, slot, so_sem.at[0], so_sem.at[1], other)

    for i in range(NA):
        for way in range(2):
            for e in range(2):
                in_head(way * NS + 2 * i + e).wait()
            ag(way, i, 0).start()
    shard(c).start()
    for k in range(Z):
        in_hid(k).start()
    for b in range(NB):
        in_tgt(b).start()
    @pl.loop(0, NB)
    def _(b):
        zed[b] = jnp.zeros((T, W), F32)

    @pl.loop(0, Z)
    def _(k):
        in_hid(k).wait()
        hid_t[k] = hid[k].T

    def column(row):
        return jnp.broadcast_to(row, (128, T)).T

    in_ids.wait()
    ids_c[...] = column(ids_ref[...].astype(F32))

    def reset():
        run_m[...] = jnp.full((T, 128), LOW, F32)
        run_s[...] = jnp.zeros((T, 128), F32)

    reset()
    own_t[...] = jnp.zeros((ROWS, W), F32)
    lsum[...] = jnp.zeros((ROWS, W), F32)

    def groups(v):
        return [v[:, g * 128 : (g + 1) * 128] for g in range(G)]

    def rowwise(step):
        @pl.loop(0, T // (ROWS * UNROLL))
        def _(k):
            for u in range(UNROLL):
                step(pl.ds(pl.multiple_of((k * UNROLL + u) * ROWS, ROWS), ROWS))

    def stats(load):
        @rowwise
        def _(at):
            cols = groups(load(at))
            old = run_m[at]
            new = functools.reduce(jnp.maximum, cols, old)
            total = run_s[at] * jnp.exp(old - new)
            run_s[at] = total + functools.reduce(jnp.add, [jnp.exp(v - new) for v in cols])
            run_m[at] = new

    def local_stats():
        m = run_m[...].T
        top = jnp.max(m, axis=0, keepdims=True)
        return top, jnp.sum(run_s[...].T * jnp.exp(m - top), axis=0, keepdims=True)

    def st(ref, s, r, k):
        return remote(ref.at[me], ref.at[me], s.at[k], r.at[me], plane(k)[1])

    def st_in(ref, s, r, k):
        j, device = plane(k)
        return remote(ref.at[j], ref.at[j], s.at[k], r.at[j], device)

    def send_stats(ref, s, r):
        top, total = local_stats()
        ref[me] = jnp.concatenate([top, total], axis=0)
        for k in range(1, NV):
            st(ref, s, r, k).start()

    def joined_stats(ref, s, r):
        for k in range(1, NV):
            st_in(ref, s, r, k).wait_recv()
        rows = [ref[j] for j in range(NV)]
        top = functools.reduce(jnp.maximum, [v[0:1] for v in rows])
        return top, functools.reduce(jnp.add, [v[1:2] * jnp.exp(v[0:1] - top) for v in rows])

    lane = lax.broadcasted_iota(jnp.int32, (ROWS, W), 1)

    def wide(v):
        return jnp.concatenate([v] * G, axis=1)

    def fill_base(b):
        col = (lane + (me * V + b * W)).astype(F32)

        @rowwise
        def _(at):
            t = tgt[b, at].astype(F32)
            p = jnp.exp(t - wide(m_c[at])) * wide(s_c[at])
            own = col == wide(ids_c[at])
            base[b, at] = jnp.where(own, p + CE, p)
            own_t[...] += jnp.where(own, t, 0.0)

    def draft(s, b, way):
        chips = (chip_at(way, s - 1), chip_at(way, s))
        lhs = jnp.concatenate([hid[k] for k in chips], axis=1)
        rhs = jnp.concatenate([hg[2 * k + e, b] for k in chips for e in range(2)], axis=0)
        zed[b] += jnp.dot(lhs, rhs, preferred_element_type=F32)

    for b in range(NB):
        in_tgt(b).wait()
    shard(sib).wait_recv()

    @pl.loop(0, NG + 1)
    def _(n):
        s = n // NA + 1
        i = lax.rem(n, NA)

        @pl.when(n < NG)
        def _():
            for way in range(2):
                ag(way, n, s).wait_recv()

                @pl.when(n + NA < NG)
                def _():
                    ag(way, n + NA, s).start()

                @pl.when(n + NA >= NG)
                def _():
                    for e in range(2):
                        al(way, 2 * i + e, s).start()

                sb(way, n, c).start()

        @pl.when(n > 0)
        def _():
            m = n - 1
            for way in range(2):
                sb(way, m, sib).wait_recv()

            @pl.when(lax.rem(m // NA, 2) == 0)
            def _():
                @pl.loop(0, 2)
                def _(e):
                    for way in range(2):
                        draft(m // NA + 1, way * NS + 2 * lax.rem(m, NA) + e, way)

        @pl.when(s == 2)
        def _():
            @pl.loop(0, 2)
            def _(e):
                for way in range(2):
                    stats(lambda at: tgt[way * NS + 2 * i + e, at].astype(F32))

        word(n)

        @pl.when(n == X + Y - 1)
        def _():
            @pl.when(me > 0)
            def _():
                pl.semaphore_wait(ready.at[2], 1)

            send_stats(st_t, tt_s, tt_r)
            reset()

        @pl.when(n == X + Y + 1)
        def _():
            top, total = joined_stats(st_t, tt_s, tt_r)
            m_c[...] = column(top)
            s_c[...] = column(1.0 / total)
            row_t[...] = top + jnp.log(total)

        @pl.when(s == Z - 2)
        def _():
            @pl.loop(0, 2)
            def _(e):
                for way in range(2):
                    fill_base(way * NS + 2 * i + e)

    @pl.loop(0, NS + 1)
    def _(i):
        @pl.when(i < NS)
        def _():
            for way in range(2):
                al(way, i, Z - 1).wait_recv()
                sl(way, i, c).start()

        @pl.when(i > 0)
        def _():
            for way in range(2):
                sl(way, i - 1, sib).wait_recv()
            for way in range(2):
                b = way * NS + i - 1
                draft(Z - 1, b, way)
                stats(lambda at: zed[b, at])

    send_stats(st_z, zz_s, zz_r)
    top_z, total_z = joined_stats(st_z, zz_s, zz_r)
    m_c[...] = column(top_z)
    s_c[...] = column((1.0 + CE) / total_z)
    row_t[...] = ((1.0 + CE) * (top_z + jnp.log(total_z)) - row_t[...]) * (1.0 / NV)

    def fill_slope(b):
        @rowwise
        def _(at):
            q = jnp.exp(zed[b, at] - wide(m_c[at])) * wide(s_c[at])
            slope[b, at] = (q - base[b, at]).astype(BF16)

    def rl(way, i):
        return remote(
            ring_out.at[way, 0, i], ring_in.at[way, 0, i], rl_s.at[way, i], rl_r.at[way, i], toward[way]
        )

    def bl(way, i):
        return remote(
            sib_out.at[way, 0, i], sib_in.at[way, 0, i], bl_s.at[way, i], bl_r.at[way, i], other
        )

    def both(n):
        return n // NA, pl.ds(2 * lax.rem(n, NA), 2)

    def rs(way, n):
        at = both(n)
        return remote(
            ring_out.at[way, *at], ring_in.at[way, *at], rs_s.at[way, n], rs_r.at[way, n], toward[way]
        )

    def rb(way, n):
        at = both(n)
        return remote(
            sib_out.at[way, *at], sib_in.at[way, *at], rb_s.at[way, n], rb_r.at[way, n], other
        )

    def product(way, s, i, own):
        got = jnp.dot(
            hid_t[chip_at(way, s + 1)], slope[way * NS + i], preferred_element_type=F32
        )
        own[0] = got[:RB]
        own[1] = got[RB:]
        sib_out[way, s, i] = own[sib].astype(BF16)

    def compute(n):
        for way in range(2):
            for e in range(2):
                product(way, n // NA, 2 * lax.rem(n, NA) + e, part.at[lax.rem(n, 2), way, e])
            rb(way, n).start()

    def finish_first(i):
        for way in range(2):
            bl(way, i).wait_recv()
            val = part[lax.rem(i, 2), way, 0, c] + sib_in[way, 0, i].astype(F32)
            ring_out[way, 0, i] = val.astype(BF16)
            rl(way, i).start()

    def finish(n):
        s = n // NA
        first = 2 * lax.rem(n, NA)
        own = part.at[lax.rem(n, 2)]
        for way in range(2):
            rb(way, n).wait_recv()
            for e in range(2):
                own[way, e, c] += sib_in[way, s, first + e].astype(F32)

        def joined(way, e):
            return own[way, e, c] + ring_in[way, s - 1, first + e].astype(F32)

        for way in range(2):

            @pl.when(s == 1)
            def _():
                for e in range(2):
                    rl(way, first + e).wait_recv()

            @pl.when(s > 1)
            def _():
                rs(way, n - NA).wait_recv()

            @pl.when(s < Z - 1)
            def _():
                for e in range(2):
                    ring_out[way, s, first + e] = joined(way, e).astype(BF16)
                rs(way, n).start()

            @pl.when(s == Z - 1)
            def _():
                for e in range(2):
                    at = pl.ds(pl.multiple_of((way * NS + first + e) * W, W), W)
                    gw_out[:, at] = joined(way, e)

    def gh(j):
        device = {"voc_0": j // Y, "voc_1": lax.rem(j, Y)}
        return remote(gh_send.at[j], gh_recv.at[me], gh_s.at[j], gh_r.at[me], device)

    def gh_in(k):
        j, device = plane(k)
        return remote(gh_send.at[j], gh_recv.at[j], gh_s.at[j], gh_r.at[j], device)

    def hidden_part(e):
        r = lax.rem(e // 4 + me // 4, NV // 4)
        q = lax.rem(e, 4)
        got = []
        for k in range(NB // 4):
            b = q * (NB // 4) + k
            lhs = jnp.concatenate([hg[4 * r + i, b] for i in range(4)], axis=0)
            got.append(
                lax.dot_general(
                    lhs, slope[b], (((1,), (1,)), ((), ())), preferred_element_type=F32
                )
            )
        got = functools.reduce(jnp.add, got)

        @pl.when(q == 0)
        def _():
            gh_acc[...] = got

        @pl.when(q > 0)
        def _():
            gh_acc[...] += got

        @pl.when(q == 3)
        def _():
            for i in range(4):
                gh_send[4 * r + i] = gh_acc[i * RB : (i + 1) * RB].astype(BF16)

                @pl.when(4 * r + i != me)
                def _():
                    gh(4 * r + i).start()

    def loss_part(b):
        @rowwise
        def _(at):
            lsum[...] += base[b, at] * (tgt[b, at].astype(F32) - zed[b, at])

    def total_of(v):
        return jnp.sum(jnp.sum(v, axis=0, keepdims=True), axis=1, keepdims=True)

    def sib_loss():
        return remote(l_sib.at[0], l_sib.at[1], lb_sem.at[0], lb_sem.at[1], other)

    def ring_loss(k):
        slot = l_z.at[chip_at(0, k)]
        return remote(slot, slot, lz_s.at[k], lz_r.at[k], toward[0])

    def ring_loss_in(k):
        slot = l_z.at[chip_at(0, k + 1)]
        return remote(slot, slot, lz_s.at[k], lz_r.at[k], toward[0])

    def sent():
        shard(c).wait_send()

        @pl.loop(0, NG)
        def _(n):
            for way in range(2):
                ag(way, n, 0).wait_send()
                sb(way, n, c).wait_send()

        @pl.loop(0, NS)
        def _(i):
            for way in range(2):
                al(way, i, 0).wait_send()
                sl(way, i, c).wait_send()

        for k in range(1, NV):
            st(st_t, tt_s, tt_r, k).wait_send()
            st(st_z, zz_s, zz_r, k).wait_send()

    def gathered():
        loss_out[...] = functools.reduce(jnp.add, [l_z[k] for k in range(Z)]) * (
            1.0 / (2 * Z * T)
        )
        for k in range(1, NV):
            gh_in(k).wait_recv()
        gh_recv[me] = gh_send[me]

        @pl.loop(0, RB // 16)
        def _(k):
            at = pl.ds(pl.multiple_of(k * 16, 16), 16)
            gh_out[at] = functools.reduce(jnp.add, [gh_recv[j, at].astype(F32) for j in range(NV)])

        sib_loss().wait_send()

        @pl.loop(0, Z - 1)
        def _(k):
            ring_loss(k).wait_send()

        for k in range(1, NV):
            st(l_xy, lx_s, lx_r, k).wait_send()
            gh_in(k).wait_send()

    @pl.loop(0, NS)
    def _(i):
        for way in range(2):
            fill_slope(way * NS + i)
            product(way, 0, i, part.at[lax.rem(i, 2), way, 0])
            bl(way, i).start()

        @pl.when(i > 0)
        def _():
            finish_first(i - 1)

    @pl.loop(NA, NC + 1)
    def _(n):
        @pl.when(n < NC)
        def _():
            compute(n)

        @pl.when(n == NA)
        def _():
            finish_first(NS - 1)

        @pl.when(n > NA)
        def _():
            finish(n - 1)

        @pl.when(n == NA + 1)
        def _():
            sent()

        @pl.when((n > NA) & (n <= NA + 2))
        def _():
            @pl.loop(0, NB // 2)
            def _(k):
                loss_part((n - NA - 1) * (NB // 2) + k)

        @pl.when(n == NA + 3)
        def _():
            local = total_of(lsum[...] - CE * own_t[...]) + total_of(row_t[...])
            l_xy[me] = jnp.broadcast_to(local, (8, 128))
            for k in range(1, NV):
                st(l_xy, lx_s, lx_r, k).start()

        @pl.when((n >= NA + 3) & (n < NA + 3 + NV // 2))
        def _():
            @pl.loop(0, 2)
            def _(e):
                hidden_part(2 * (n - NA - 3) + e)

        @pl.when(n == NA + 4)
        def _():
            for k in range(1, NV):
                st_in(l_xy, lx_s, lx_r, k).wait_recv()
            l_sib[0] = functools.reduce(jnp.add, [l_xy[j] for j in range(NV)])
            sib_loss().start()

        @pl.when(n == NA + 5)
        def _():
            sib_loss().wait_recv()
            l_z[z] = l_sib[0] + l_sib[1]
            ring_loss(0).start()

        @pl.when((n > NA + 5) & (n <= NA + 5 + Z - 1))
        def _():
            k = n - NA - 5
            ring_loss_in(k - 1).wait_recv()

            @pl.when(k < Z - 1)
            def _():
                ring_loss(k).start()

        @pl.when(n == NC - 1)
        def _():
            gathered()

    @pl.loop(0, NS)
    def _(i):
        for way in range(2):
            rl(way, i).wait_send()
            bl(way, i).wait_send()

    @pl.loop(NA, NC - NA)
    def _(n):
        for way in range(2):
            rs(way, n).wait_send()

    @pl.loop(NA, NC)
    def _(n):
        for way in range(2):
            rb(way, n).wait_send()


def hand_over(loss, gh, gw, loss_out, gh_out, gw_out, sems):
    copies = [
        pltpu.make_async_copy(src, dst, sems.at[k])
        for k, (src, dst) in enumerate(((gw, gw_out), (gh, gh_out)))
    ]
    for copy in copies:
        copy.start()
    loss_out[...] = loss[0:1, 0:1]
    for copy in copies:
        copy.wait()


def body(dims, hidden, head, target, ids):
    Z, X, Y, T, D, V, NS = dims
    NV = X * Y
    NB = 2 * NS
    W = V // NB
    RB = D // (2 * Z)
    NA = NS // 2
    NC, NG = Z * NA, (Z - 2) * NA
    vmem, dma = pltpu.VMEM, pltpu.SemaphoreType.DMA
    hbm = pl.BlockSpec(memory_space=pltpu.HBM)
    local = pl.BlockSpec(memory_space=pltpu.VMEM)
    loss, gh, gw = pl.pallas_call(
        functools.partial(kernel, dims),
        out_shape=(
            vmem((8, 128), F32),
            vmem((RB, T), F32),
            vmem((RB, V), F32),
        ),
        in_specs=[hbm, hbm, hbm, hbm],
        out_specs=(local, local, local),
        scratch_shapes=[
            vmem((1, T), jnp.int32),
            vmem((2 * Z, NB, RB, W), BF16),
            vmem((Z, T, 2 * RB), BF16),
            vmem((Z, 2 * RB, T), BF16),
            vmem((NB, T, W), BF16),
            vmem((NB, T, W), F32),
            vmem((NB, T, W), F32),
            vmem((NB, T, W), BF16),
            vmem((2, 2, 2, 2, RB, W), F32),
            vmem((2, Z, NS, RB, W), BF16),
            vmem((2, Z, NS, RB, W), BF16),
            vmem((2, Z - 1, NS, RB, W), BF16),
            vmem((2, Z - 1, NS, RB, W), BF16),
            vmem((NV, RB, T), BF16),
            vmem((NV, RB, T), BF16),
            vmem((4 * RB, T), F32),
            vmem((NV, 2, T), F32),
            vmem((NV, 2, T), F32),
            vmem((T, 128), F32),
            vmem((T, 128), F32),
            vmem((T, 128), F32),
            vmem((T, 128), F32),
            vmem((T, 128), F32),
            vmem((ROWS, W), F32),
            vmem((ROWS, W), F32),
            vmem((1, T), F32),
            vmem((NV, 8, 128), F32),
            vmem((2, 8, 128), F32),
            vmem((Z, 8, 128), F32),
            dma((2 * NB + Z + 1,)),
            pltpu.SemaphoreType.REGULAR((3,)),
            dma((2, NG)), dma((2, NG)),
            dma((2, NS)), dma((2, NS)),
            dma((2, NG)), dma((2, NG)),
            dma((2, NS)), dma((2, NS)),
            dma((2,)),
            dma((2, NS)), dma((2, NS)),
            dma((2, NC)), dma((2, NC)),
            dma((2, NS)), dma((2, NS)),
            dma((2, NC)), dma((2, NC)),
            dma((NV,)), dma((NV,)),
            dma((NV,)), dma((NV,)),
            dma((NV,)), dma((NV,)),
            dma((NV,)), dma((NV,)),
            dma((Z,)), dma((Z,)),
            dma((2,)),
        ],
        compiler_params=pltpu.CompilerParams(
            collective_id=0, has_side_effects=True, vmem_limit_bytes=60 * 1024 * 1024
        ),
        name="step",
    )(hidden, head, target, ids.reshape(1, T))
    loss, gh, gw = pl.pallas_call(
        hand_over,
        out_shape=(
            jax.ShapeDtypeStruct((1, 1), F32),
            jax.ShapeDtypeStruct((RB, T), F32),
            jax.ShapeDtypeStruct((RB, V), F32),
        ),
        in_specs=[local] * 3,
        out_specs=(local, hbm, hbm),
        scratch_shapes=[dma((3,))],
        compiler_params=pltpu.CompilerParams(vmem_limit_bytes=4 * 1024 * 1024),
        name="hand_over",
    )(loss, gh, gw)
    return loss.reshape(()), gh.T, gw


def solution(mesh):
    sizes = mesh.shape
    tok, voc = sizes["tok"], sizes["voc"]
    side = {16: 4, 8: 4, 4: 2}[voc]
    Z, X, Y = tok // 2, side, voc // side
    torus = Mesh(mesh.devices.reshape(Z, 2, X, Y), TOK + VOC)

    def whole(hidden, head, target, ids):
        dims = (Z, X, Y, hidden.shape[0] // tok, hidden.shape[1], head.shape[1] // voc, 4)
        return jax.shard_map(
            functools.partial(body, dims),
            mesh=torus,
            in_specs=(P(TOK, None), P(TOK, VOC), P(TOK, VOC), P(TOK)),
            out_specs=(P(), P(TOK, VOC), P(TOK, VOC)),
            check_vma=False,
        )(hidden, head, target, ids)

    return whole
```
